256 devices in a mesh: fsdp: 16 (over y, z_lo, core), sp: 16 (over x, z_hi).
Axes of the slice: x: 4, y: 4, z: 8 (z_hi: 4, z_lo: 2; z = z_hi * 2 + z_lo), core: 2. Of those that a mesh axis runs over, the one named last changes fastest.
Arguments:
- hidden: bfloat16 [16, 4096, 5120], P('fsdp', 'sp'), may hold values from -6 to 6
- queries: bfloat16 [16, 4096, 4096], P('fsdp', 'sp'), may hold values from -240 to 240
- norm_gain: float32 [5120], replicated, may hold values from 0.5 to 1.5
- kv_weight: bfloat16 [5120, 2048], P('fsdp'), may hold values from -0.078125 to 0.078125
- value_bias: float32 [1024], replicated, may hold values from -3 to 3
- doc_lengths: int32 [16, 16], P('fsdp'), may hold values from 1 to 1024, 4096 in all within a row
Outputs:
- attended: bfloat16 [16, 4096, 4096], P('fsdp', 'sp')
The draws below stay inside these ranges and needn't reach their ends.
Inputs may be any that keep to these rules, and one draw needn't show every extreme that they name: `doc_lengths`: each row sums to 4096 and its largest entry is 1024.
All inputs are finite; a program needn't handle non-finite values.
Results may differ from the reference program's by a relative error of at most 0.0067.
Values may be sent and summed in bfloat16 or wider, within the bound.
A program may use at most 128 MiB of HBM per device.

```python
import math
import jax
import jax.numpy as jnp
import numpy as np
from jax import lax

D = 5120
QH = 32
KVH = 8
HD = 128
NDOC = 16
GROUPS = 16
SEQ = 4096
MOST = 1024


def draw_queries(key, part):
    drawn = jnp.clip(jax.random.normal(key, (GROUPS, SEQ, QH * HD), jnp.float32), -6.0, 6.0)
    return drawn.astype(jnp.bfloat16)


def steps_of(rng, extent, shards, low, high):
    loudness, own = 1.0, jax.random.fold_in(rng, 6)
    for position, parts in shards:
        steps = jnp.exp(jax.random.uniform(jax.random.fold_in(own, position), (parts,), jnp.float32, low / len(shards), high / len(shards)))
        loudness = loudness * jnp.repeat(steps, extent[position] // parts).reshape([-1 if axis == position else 1 for axis in range(len(extent))])
    return loudness


def split_up(number_of, total, bound, lean):
    portions = [(1 << 20) // math.isqrt(standing ** lean) + 1 for standing in range(2, number_of + 1)]
    spare, given = total - bound - (number_of - 1), [1] * (number_of - 1)
    while spare > 0:
        movable = [i for i in range(number_of - 1) if given[i] < bound]
        whole, remaining = sum([portions[i] for i in movable]), spare
        for i in movable:
            addition = min(bound - given[i], max(1, remaining * portions[i] // whole), spare)
            given[i] = given[i] + addition
            spare = spare - addition
    return np.array([bound] + given)


def uneven(key, count, total, reach, skew):
    if count == 2:
        one = jax.random.randint(key, (), max(1, total - reach), min(reach, total - 1) + 1)
        return jnp.stack([one, total - one])
    sizes = jnp.asarray(split_up(count, total, reach, skew), jnp.int32)
    couples = (count - 1) // 2
    donor, taker = sizes[1:1 + 2 * couples:2], sizes[2:2 + 2 * couples:2]
    room = jnp.minimum(donor - 1, reach - taker)
    shifted = jax.random.randint(jax.random.fold_in(key, 1), (couples,), 0, 1 << 20) % (room + 1)
    sizes = sizes.at[1:1 + 2 * couples:2].set(donor - shifted).at[2:2 + 2 * couples:2].set(taker + shifted)
    return sizes[jax.random.permutation(jax.random.fold_in(key, 2), count)]


def gaussian(key, shape, width, most, cuts=(), kind=jnp.bfloat16):
    values = jax.random.normal(key, shape, jnp.float32) * width
    if len(cuts) > 0:
        values = steps_of(key, shape, cuts, -0.22, 0.18) * values
    return jnp.clip(values, min=-most, max=most).astype(kind)


def setup_inputs(seed: int = 0) -> dict:
    seeds = jax.random.split(jax.random.key(seed), 7)
    hidden = gaussian(seeds[0], (GROUPS, SEQ, D), 1.0, 6.0, ((0, 16), (1, 16)))
    queries = draw_queries(jax.random.fold_in(seeds[6], 71), 0)
    norm_gain = jnp.clip(1.0 + 0.1 * jax.random.normal(seeds[2], (D,), jnp.float32), 0.5, 1.5)
    kv_weight = gaussian(seeds[3], (D, 2 * KVH * HD), D ** -0.5, 0.078125, ((0, 16),))
    value_bias = gaussian(seeds[4], (KVH * HD,), 0.5, 3.0, (), jnp.float32)
    doc_lengths = jax.vmap(lambda own: uneven(own, NDOC, SEQ, MOST, 2))(jax.random.split(seeds[5], GROUPS)).reshape((GROUPS, NDOC)).astype(jnp.int32)
    return {"hidden": hidden, "queries": queries, "norm_gain": norm_gain, "kv_weight": kv_weight, "value_bias": value_bias, "doc_lengths": doc_lengths}


EPS = 1e-06

def attend(query_all, key_all, value_all, doc_ids):
    length = query_all.shape[0]
    block = min(512, length)
    longest = length // 4
    window = min(length, block + longest)
    scale = HD ** (-0.5)

    def one_block(index):
        first = (index * block).astype(jnp.int32)
        start = jnp.clip(first - longest, 0, length - window).astype(jnp.int32)
        query_block = lax.dynamic_slice_in_dim(query_all, first, block, 0).astype(jnp.float32)
        key_block = lax.dynamic_slice_in_dim(key_all, start, window, 0).astype(jnp.float32)
        value_block = lax.dynamic_slice_in_dim(value_all, start, window, 0).astype(jnp.float32)
        query_ids = lax.dynamic_slice_in_dim(doc_ids, first, block, 0)
        key_ids = lax.dynamic_slice_in_dim(doc_ids, start, window, 0)
        query_pos = first + jnp.arange(block, dtype=jnp.int32)
        key_pos = start + jnp.arange(window, dtype=jnp.int32)
        allowed = (key_pos[None, :] <= query_pos[:, None]) & (key_ids[None, :] == query_ids[:, None])
        scores = jnp.einsum('qnd,knd->nqk', query_block, key_block) * scale
        scores = jnp.where(allowed[None], scores, -jnp.inf)
        highest = lax.optimization_barrier(jnp.max(scores, axis=-1, keepdims=True))
        probs = jnp.exp(scores - highest)
        probs = (probs / lax.optimization_barrier(jnp.sum(probs, axis=-1, keepdims=True))).astype(jnp.bfloat16)
        output = jnp.einsum('nqk,knd->qnd', probs.astype(jnp.float32), value_block)
        return output.astype(jnp.bfloat16)
    blocks = lax.map(one_block, jnp.arange(length // block, dtype=jnp.int32))
    return blocks.reshape(length, query_all.shape[1], query_all.shape[2])

def reference(hidden, queries, norm_gain, kv_weight, value_bias, doc_lengths):
    wide = hidden.astype(jnp.float32)
    normed = (wide * lax.rsqrt(lax.optimization_barrier(jnp.mean(wide * wide, axis=-1, keepdims=True)) + EPS) * norm_gain).astype(jnp.bfloat16)
    projected = jnp.dot(normed.reshape(GROUPS * SEQ, D), kv_weight, preferred_element_type=jnp.float32)
    projected = projected.reshape(GROUPS, SEQ, 2 * KVH * HD)
    keys = projected[..., :KVH * HD].astype(jnp.bfloat16)
    values = (projected[..., KVH * HD:] + value_bias).astype(jnp.bfloat16)
    ratio = QH // KVH

    def one_group(operands):
        query_group, key_group, value_group, lengths = operands
        ends = jnp.cumsum(lengths).astype(jnp.int32)
        positions = jnp.arange(SEQ, dtype=jnp.int32)
        doc_ids = lax.optimization_barrier(jnp.sum((positions[:, None] >= ends[None, :]).astype(jnp.int32), axis=1)).astype(jnp.int32)
        query_heads = query_group.reshape(SEQ, QH, HD)
        key_heads = jnp.repeat(key_group.reshape(SEQ, KVH, HD), ratio, axis=1)
        value_heads = jnp.repeat(value_group.reshape(SEQ, KVH, HD), ratio, axis=1)
        return attend(query_heads, key_heads, value_heads, doc_ids).reshape(SEQ, QH * HD)
    return lax.map(one_group, (queries, keys, values, doc_lengths))
```

```python
import jax
import jax.numpy as jnp
from jax import lax
from jax.experimental import pallas as pl
from jax.experimental.pallas import tpu as pltpu
from jax.sharding import PartitionSpec as P

QH = 32
KVH = 8
HD = 128
D = 5120
T = 256
NDOC = 16
RATIO = QH // KVH
ROWS = D // 16
QUART = ROWS // 4
WIN = 5 * T
EPS = 1e-06
LOG2E = 1.4426950408889634
MESH = pl.DeviceIdType.MESH

YA, ZA, YB, XC, EC, XP, ZU, ZD, RU, RD = 0, 3, 4, 7, 10, 11, 12, 13, 14, 15
KINDS = 16


def kernel(
    dl_ref, hid_hbm, q_hbm, gain_ref, w_hbm, vb_ref, out_hbm,
    wbuf, nbuf, qbuf, kvbuf, bias, obuf,
    w_sem, in_sem, out_sem, send, recv,
):
    f = lax.axis_index("fsdp")
    s = lax.axis_index("sp")
    y, zl, c = f // 4, lax.rem(f // 2, 2), lax.rem(f, 2)
    x, zh = s // 4, lax.rem(s, 4)

    def dev(yy, zz, cc, xx, hh):
        return {"fsdp": (yy * 2 + zz) * 2 + cc, "sp": xx * 4 + hh}

    def y_at(d):
        return dev(lax.rem(y + d, 4), zl, c, x, zh)

    def x_at(d):
        return dev(y, zl, c, lax.rem(x + d, 4), zh)

    def h_at(d):
        return dev(y, zl, c, x, lax.rem(zh + d, 4))

    z_pair = dev(y, 1 - zl, c, x, zh)
    core_pair = dev(y, zl, 1 - c, x, zh)
    quarter = pl.ds(pl.multiple_of(x * QUART, 16), QUART)

    def remote(src, dst, kind, h, device, recv_kind=None):
        return pltpu.make_async_remote_copy(
            src_ref=src,
            dst_ref=dst,
            send_sem=send.at[kind, h],
            recv_sem=recv.at[kind if recv_kind is None else recv_kind, h],
            device_id=device,
            device_id_type=MESH,
        )

    def ya(h, d):
        own = wbuf.at[h, y, zl, c]
        return remote(own, own, YA + d - 1, h, y_at(d))

    def za(h):
        part = wbuf.at[h, y, zl, c, quarter]
        return remote(part, part, ZA, h, z_pair)

    def yb(h, d):
        part = wbuf.at[h, y, 1 - zl, c, quarter]
        return remote(part, part, YB + d - 1, h, y_at(d))

    def xc(h, d):
        part = wbuf.at[h, :, 1 - zl, c, quarter]
        return remote(part, part, XC + d - 1, h, x_at(d))

    def ec(h):
        half = wbuf.at[h, :, :, c]
        return remote(half, half, EC, h, core_pair)

    def xp(h):
        return remote(kvbuf.at[h, 4], kvbuf.at[h, 0], XP, h, x_at(1))

    def zu(h):
        return remote(kvbuf.at[h, jnp.where(zh < 3, 4, 0)], kvbuf.at[h, 3], ZU, h, h_at(1))

    def zd(h):
        return remote(kvbuf.at[h, jnp.where(zh > 0, 0, 4)], kvbuf.at[h, 1], ZD, h, h_at(3))

    def ru(h):
        return remote(kvbuf.at[h, 3], kvbuf.at[h, 2], RU, h, h_at(1), RU)

    def rd(h):
        return remote(kvbuf.at[h, 1], kvbuf.at[h, 2], RD, h, h_at(3), RU)

    def w_local(h, part):
        columns = pl.ds(pl.multiple_of(part * KVH * HD + h * HD, HD), HD)
        return pltpu.make_async_copy(
            w_hbm.at[:, columns],
            wbuf.at[h, y, zl, c, :, pl.ds(part * HD, HD)],
            w_sem.at[part, h],
        )

    def out_copy(h):
        columns = pl.ds(pl.multiple_of(h * RATIO * HD, HD), RATIO * HD)
        return pltpu.make_async_copy(obuf.at[:, columns], out_hbm.at[:, columns], out_sem.at[h])

    hid_copy = pltpu.make_async_copy(hid_hbm, nbuf, in_sem.at[0])
    q_copy = pltpu.make_async_copy(q_hbm, qbuf, in_sem.at[1])

    @pl.loop(0, KVH)
    def _(h):
        w_local(h, 0).start()
        w_local(h, 1).start()

    hid_copy.start()
    q_copy.start()

    barrier = pltpu.get_barrier_semaphore()
    partners = [y_at(1), y_at(2), y_at(3), x_at(1), x_at(2), x_at(3), h_at(1), h_at(3), z_pair, core_pair]
    for device in partners:
        pl.semaphore_signal(barrier, inc=1, device_id=device, device_id_type=MESH)
    pl.semaphore_wait(barrier, len(partners))

    def start_a(h):
        w_local(h, 0).wait()
        w_local(h, 1).wait()
        za(h).start()
        for d in (1, 3, 2):
            ya(h, d).start()

    def start_b(h):
        za(h).wait_recv()
        for d in (1, 3, 2):
            yb(h, d).start()

    def start_c(h):
        for d in (1, 2, 3):
            yb(h, d).wait_recv()
        for d in (1, 3, 2):
            xc(h, d).start()

    def start_e(h):
        for d in (1, 2, 3):
            ya(h, d).wait_recv()
        for d in (1, 2, 3):
            xc(h, d).wait_recv()
        ec(h).start()

    def project(h):
        ec(h).wait_recv()
        weight = wbuf[h].reshape(D, 2 * HD)
        result = jnp.dot(nbuf[...], weight, preferred_element_type=jnp.float32)
        kvbuf[h, 4, :, pl.ds(0, HD)] = result[:, :HD].astype(jnp.bfloat16)
        kvbuf[h, 4, :, pl.ds(HD, HD)] = (result[:, HD:] + vb_ref[pl.ds(h, 1), :]).astype(jnp.bfloat16)

    def attend(h, first_head, count):
        key = kvbuf[h, :, :, pl.ds(0, HD)].reshape(WIN, HD)
        value = kvbuf[h, :, :, pl.ds(HD, HD)].reshape(WIN, HD)
        for r in range(first_head, first_head + count):
            columns = pl.ds(pl.multiple_of((h * RATIO + r) * HD, HD), HD)
            scores = lax.dot_general(
                qbuf[:, columns], key, (((1,), (1,)), ((), ())), preferred_element_type=jnp.float32
            )
            scores = scores * (HD**-0.5 * LOG2E) + bias[...]
            highest = jnp.max(scores, axis=-1, keepdims=True)
            probs = jnp.exp2(scores - highest)
            total = jnp.sum(probs, axis=-1, keepdims=True)
            output = jnp.dot(probs.astype(jnp.bfloat16), value, preferred_element_type=jnp.float32)
            obuf[:, columns] = (output / total).astype(jnp.bfloat16)

    start_a(0)

    hid_copy.wait()

    @pl.loop(0, T // 16)
    def _(i):
        rows = pl.ds(pl.multiple_of(i * 16, 16), 16)
        wide = nbuf[rows, :].astype(jnp.float32)
        square = jnp.mean(wide * wide, axis=-1, keepdims=True)
        nbuf[rows, :] = (wide * lax.rsqrt(square + EPS) * gain_ref[...]).astype(jnp.bfloat16)

    start_b(0)
    start_a(1)

    first = s * T
    query_pos = first + lax.broadcasted_iota(jnp.int32, (T, 1), 0)
    begin = jnp.zeros((T, 1), jnp.int32)
    end = dl_ref[0, 0]
    for d in range(NDOC):
        begin = jnp.where(query_pos >= end, end, begin)
        if d + 1 < NDOC:
            end = end + dl_ref[0, d + 1]
    key_pos = first - 4 * T + lax.broadcasted_iota(jnp.int32, (T, WIN), 1)
    bias[...] = jnp.where((key_pos <= query_pos) & (key_pos >= begin), 0.0, -jnp.inf)

    start_c(0)
    q_copy.wait()

    @pl.loop(0, KVH + 2)
    def _(i):
        @pl.when(i < KVH)
        def _():
            start_e(i)

        @pl.when(i + 1 < KVH)
        def _():
            start_b(i + 1)

        @pl.when(i >= 2)
        def _():
            ru(i - 2).wait_recv()
            attend(i - 2, 0, 2)

        @pl.when(i < KVH)
        def _():
            project(i)
            xp(i).start()

            @pl.when(zh < 3)
            def _():
                zu(i).start()

            @pl.when(zh == 0)
            def _():
                zd(i).start()

        @pl.when(i + 1 < KVH)
        def _():
            start_c(i + 1)

        @pl.when(i + 2 < KVH)
        def _():
            start_a(i + 2)

        @pl.when(i >= 2)
        def _():
            attend(i - 2, 2, 2)
            out_copy(i - 2).start()

        @pl.when(i < KVH)
        def _():
            xp(i).wait_recv()

            @pl.when(zh == 3)
            def _():
                zu(i).start()

            @pl.when(zh > 0)
            def _():
                zd(i).start()

        @pl.when((i >= 1) & (i <= KVH))
        def _():
            zu(i - 1).wait_recv()
            zd(i - 1).wait_recv()

            @pl.when((zh == 1) | (zh == 2))
            def _():
                ru(i - 1).start()
                rd(i - 1).start()

    @pl.loop(0, KVH)
    def _(h):
        for d in (1, 2, 3):
            ya(h, d).wait_send()
            yb(h, d).wait_send()
            xc(h, d).wait_send()
        za(h).wait_send()
        ec(h).wait_send()
        xp(h).wait_send()
        zu(h).wait_send()
        zd(h).wait_send()

        @pl.when((zh == 1) | (zh == 2))
        def _():
            ru(h).wait_send()
            rd(h).wait_send()

        out_copy(h).wait()


def shards(hidden, queries, norm_gain, kv_weight, value_bias, doc_lengths):
    anywhere = pl.BlockSpec(memory_space=pl.ANY)
    vmem = pl.BlockSpec(memory_space=pltpu.VMEM)
    out = pl.pallas_call(
        kernel,
        out_shape=jax.ShapeDtypeStruct((T, QH * HD), jnp.bfloat16),
        in_specs=[pl.BlockSpec(memory_space=pltpu.SMEM), anywhere, anywhere, vmem, anywhere, vmem],
        out_specs=anywhere,
        scratch_shapes=[
            pltpu.VMEM((KVH, 4, 2, 2, ROWS, 2 * HD), jnp.bfloat16),
            pltpu.VMEM((T, D), jnp.bfloat16),
            pltpu.VMEM((T, QH * HD), jnp.bfloat16),
            pltpu.VMEM((KVH, 5, T, 2 * HD), jnp.bfloat16),
            pltpu.VMEM((T, WIN), jnp.float32),
            pltpu.VMEM((T, QH * HD), jnp.bfloat16),
            pltpu.SemaphoreType.DMA((2, KVH)),
            pltpu.SemaphoreType.DMA((2,)),
            pltpu.SemaphoreType.DMA((KVH,)),
            pltpu.SemaphoreType.DMA((KINDS, KVH)),
            pltpu.SemaphoreType.DMA((KINDS, KVH)),
        ],
        compiler_params=pltpu.CompilerParams(
            collective_id=0, has_side_effects=True, vmem_limit_bytes=60 * 1024 * 1024
        ),
    )(
        doc_lengths,
        hidden[0],
        queries[0],
        norm_gain.reshape(1, D),
        kv_weight,
        value_bias.reshape(KVH, HD),
    )
    return out.reshape(1, T, QH * HD)


def solution(mesh):
    in_specs = (
        P("fsdp", "sp", None),
        P("fsdp", "sp", None),
        P(),
        P("fsdp", None),
        P(),
        P("fsdp", None),
    )
    out_specs = P("fsdp", "sp", None)
    return jax.shard_map(shards, mesh=mesh, in_specs=in_specs, out_specs=out_specs, check_vma=False)
```

```python
import jax
import jax.numpy as jnp
from jax import lax
from jax.experimental import pallas as pl
from jax.experimental.pallas import tpu as pltpu
from jax.sharding import PartitionSpec as P

QH = 32
KVH = 8
HD = 128
D = 5120
T = 256
NDOC = 16
RATIO = QH // KVH
ROWS = D // 16
QUART = ROWS // 4
WIN = 5 * T
EPS = 1e-06
LOG2E = 1.4426950408889634
MESH = pl.DeviceIdType.MESH

YA, ZA, YB, XC, EC, XP, ZU, ZD, ZT = 0, 3, 4, 7, 10, 11, 12, 13, 14
KINDS = 15


def kernel(
    dl_ref, hid_hbm, q_hbm, gain_ref, w_hbm, vb_ref, out_hbm,
    wbuf, nbuf, qbuf, kvbuf, bias, obuf,
    w_sem, in_sem, out_sem, send, recv,
):
    f = lax.axis_index("fsdp")
    s = lax.axis_index("sp")
    y, zl, c = f // 4, lax.rem(f // 2, 2), lax.rem(f, 2)
    x, zh = s // 4, lax.rem(s, 4)

    def dev(yy, zz, cc, xx, hh):
        return {"fsdp": (yy * 2 + zz) * 2 + cc, "sp": xx * 4 + hh}

    def y_at(d):
        return dev(lax.rem(y + d, 4), zl, c, x, zh)

    def x_at(d):
        return dev(y, zl, c, lax.rem(x + d, 4), zh)

    def h_at(d):
        return dev(y, zl, c, x, lax.rem(zh + d, 4))

    z_pair = dev(y, 1 - zl, c, x, zh)
    z_beside = lax.rem(zh + 3 + 2 * zl, 4)
    z_other = dev(y, 1 - zl, c, x, z_beside)
    core_pair = dev(y, zl, 1 - c, x, zh)
    quarter = pl.ds(pl.multiple_of(x * QUART, 16), QUART)

    def remote(src, dst, kind, h, device):
        return pltpu.make_async_remote_copy(
            src_ref=src,
            dst_ref=dst,
            send_sem=send.at[kind, h],
            recv_sem=recv.at[kind, h],
            device_id=device,
            device_id_type=MESH,
        )

    def ya(h, d):
        own = wbuf.at[h, y, zl, c]
        return remote(own, own, YA + d - 1, h, y_at(d))

    def za(h):
        part = wbuf.at[h, y, zl, c, quarter]
        return remote(part, part, ZA, h, dev(y, 1 - zl, c, x, jnp.where(lax.rem(h, 2) == 0, zh, z_beside)))

    def yb(h, d):
        part = wbuf.at[h, y, 1 - zl, c, quarter]
        return remote(part, part, YB + d - 1, h, y_at(d))

    def xc(h, d):
        part = wbuf.at[h, :, 1 - zl, c, quarter]
        return remote(part, part, XC + d - 1, h, x_at(d))

    def ec(h):
        half = wbuf.at[h, :, :, c]
        return remote(half, half, EC, h, core_pair)

    def xp(h):
        return remote(kvbuf.at[h, 4], kvbuf.at[h, 0], XP, h, x_at(1))

    def zu(h):
        return remote(kvbuf.at[h, jnp.where(zh < 3, 4, 0)], kvbuf.at[h, 3], ZU, h, h_at(1))

    def zd(h):
        return remote(kvbuf.at[h, jnp.where(zh > 0, 0, 4)], kvbuf.at[h, 1], ZD, h, h_at(3))

    def zt(h):
        return remote(kvbuf.at[h, jnp.where(zh < 2, 4, 0)], kvbuf.at[h, 2], ZT, h, h_at(2))

    def w_local(h, part):
        columns = pl.ds(pl.multiple_of(part * KVH * HD + h * HD, HD), HD)
        return pltpu.make_async_copy(
            w_hbm.at[:, columns],
            wbuf.at[h, y, zl, c, :, pl.ds(part * HD, HD)],
            w_sem.at[part, h],
        )

    def out_copy(h):
        columns = pl.ds(pl.multiple_of(h * RATIO * HD, HD), RATIO * HD)
        return pltpu.make_async_copy(obuf.at[:, columns], out_hbm.at[:, columns], out_sem.at[h])

    hid_copy = pltpu.make_async_copy(hid_hbm, nbuf, in_sem.at[0])
    q_copy = pltpu.make_async_copy(q_hbm, qbuf, in_sem.at[1])

    @pl.loop(0, KVH)
    def _(h):
        w_local(h, 0).start()
        w_local(h, 1).start()

    hid_copy.start()
    q_copy.start()

    barrier = pltpu.get_barrier_semaphore()
    partners = [y_at(1), y_at(2), y_at(3), x_at(1), x_at(2), x_at(3), h_at(1), h_at(2), h_at(3), z_pair, z_other, core_pair]
    for device in partners:
        pl.semaphore_signal(barrier, inc=1, device_id=device, device_id_type=MESH)
    pl.semaphore_wait(barrier, len(partners))

    def start_a(h, offsets=(1, 3, 2)):
        w_local(h, 0).wait()
        w_local(h, 1).wait()
        za(h).start()
        for d in offsets:
            ya(h, d).start()

    def start_b(h):
        za(h).wait_recv()
        for d in (1, 3, 2):
            yb(h, d).start()

    def start_c(h):
        for d in (1, 2, 3):
            yb(h, d).wait_recv()
        for d in (1, 3, 2):
            xc(h, d).start()

    def start_e(h):
        for d in (1, 2, 3):
            ya(h, d).wait_recv()
        for d in (1, 2, 3):
            xc(h, d).wait_recv()
        ec(h).start()

    def project(h):
        ec(h).wait_recv()
        weight = wbuf[h].reshape(D, 2 * HD)
        result = jnp.dot(nbuf[...], weight, preferred_element_type=jnp.float32)
        kvbuf[h, 4, :, pl.ds(0, HD)] = result[:, :HD].astype(jnp.bfloat16)
        kvbuf[h, 4, :, pl.ds(HD, HD)] = (result[:, HD:] + vb_ref[pl.ds(h, 1), :]).astype(jnp.bfloat16)

    def send_own(h):
        xp(h).start()

        @pl.when(zh < 3)
        def _():
            zu(h).start()

        @pl.when(zh < 2)
        def _():
            zt(h).start()

        @pl.when(zh == 0)
        def _():
            zd(h).start()

    def send_previous(h):
        xp(h).wait_recv()

        @pl.when(zh > 0)
        def _():
            zd(h).start()

        @pl.when(zh >= 2)
        def _():
            zt(h).start()

        @pl.when(zh == 3)
        def _():
            zu(h).start()

    def attend(h):
        zu(h).wait_recv()
        zd(h).wait_recv()
        zt(h).wait_recv()
        key = kvbuf[h, :, :, pl.ds(0, HD)].reshape(WIN, HD)
        value = kvbuf[h, :, :, pl.ds(HD, HD)].reshape(WIN, HD)
        for r in range(RATIO):
            columns = pl.ds(pl.multiple_of((h * RATIO + r) * HD, HD), HD)
            scores = lax.dot_general(
                qbuf[:, columns], key, (((1,), (1,)), ((), ())), preferred_element_type=jnp.float32
            )
            scores = scores * (HD**-0.5 * LOG2E) + bias[...]
            highest = jnp.max(scores, axis=-1, keepdims=True)
            probs = jnp.exp2(scores - highest)
            total = jnp.sum(probs, axis=-1, keepdims=True)
            output = jnp.dot(probs.astype(jnp.bfloat16), value, preferred_element_type=jnp.float32)
            obuf[:, columns] = (output / total).astype(jnp.bfloat16)
        out_copy(h).start()

    start_a(0, (1, 3))

    first = s * T
    query_pos = first + lax.broadcasted_iota(jnp.int32, (T, 1), 0)
    begin = jnp.zeros((T, 1), jnp.int32)
    end = dl_ref[0, 0]
    for d in range(NDOC):
        begin = jnp.where(query_pos >= end, end, begin)
        if d + 1 < NDOC:
            end = end + dl_ref[0, d + 1]
    key_pos = first - 4 * T + lax.broadcasted_iota(jnp.int32, (T, WIN), 1)
    bias[...] = jnp.where((key_pos <= query_pos) & (key_pos >= begin), 0.0, -jnp.inf)

    start_b(0)
    ya(0, 2).start()
    start_a(1)
    hid_copy.wait()

    @pl.loop(0, T // 16)
    def _(i):
        rows = pl.ds(pl.multiple_of(i * 16, 16), 16)
        wide = nbuf[rows, :].astype(jnp.float32)
        square = jnp.mean(wide * wide, axis=-1, keepdims=True)
        nbuf[rows, :] = (wide * lax.rsqrt(square + EPS) * gain_ref[...]).astype(jnp.bfloat16)

    q_copy.wait()

    stages = [
        (5, send_previous),
        (4, project),
        (4, send_own),
        (3, start_e),
        (2, start_c),
        (1, start_b),
        (0, start_a),
        (8, attend),
    ]

    @pl.loop(2, KVH + 8)
    def _(i):
        for lag, stage in stages:

            @pl.when((i >= lag) & (i < KVH + lag))
            def _(lag=lag, stage=stage):
                stage(i - lag)

    @pl.loop(0, KVH)
    def _(h):
        for d in (1, 2, 3):
            ya(h, d).wait_send()
            yb(h, d).wait_send()
            xc(h, d).wait_send()
        za(h).wait_send()
        ec(h).wait_send()
        xp(h).wait_send()
        zu(h).wait_send()
        zd(h).wait_send()

        zt(h).wait_send()
        out_copy(h).wait()


def shards(hidden, queries, norm_gain, kv_weight, value_bias, doc_lengths):
    anywhere = pl.BlockSpec(memory_space=pl.ANY)
    vmem = pl.BlockSpec(memory_space=pltpu.VMEM)
    out = pl.pallas_call(
        kernel,
        out_shape=jax.ShapeDtypeStruct((T, QH * HD), jnp.bfloat16),
        in_specs=[pl.BlockSpec(memory_space=pltpu.SMEM), anywhere, anywhere, vmem, anywhere, vmem],
        out_specs=anywhere,
        scratch_shapes=[
            pltpu.VMEM((KVH, 4, 2, 2, ROWS, 2 * HD), jnp.bfloat16),
            pltpu.VMEM((T, D), jnp.bfloat16),
            pltpu.VMEM((T, QH * HD), jnp.bfloat16),
            pltpu.VMEM((KVH, 5, T, 2 * HD), jnp.bfloat16),
            pltpu.VMEM((T, WIN), jnp.float32),
            pltpu.VMEM((T, QH * HD), jnp.bfloat16),
            pltpu.SemaphoreType.DMA((2, KVH)),
            pltpu.SemaphoreType.DMA((2,)),
            pltpu.SemaphoreType.DMA((KVH,)),
            pltpu.SemaphoreType.DMA((KINDS, KVH)),
            pltpu.SemaphoreType.DMA((KINDS, KVH)),
        ],
        compiler_params=pltpu.CompilerParams(
            collective_id=0, has_side_effects=True, vmem_limit_bytes=60 * 1024 * 1024
        ),
    )(
        doc_lengths,
        hidden[0],
        queries[0],
        norm_gain.reshape(1, D),
        kv_weight,
        value_bias.reshape(KVH, HD),
    )
    return out.reshape(1, T, QH * HD)


def solution(mesh):
    in_specs = (
        P("fsdp", "sp", None),
        P("fsdp", "sp", None),
        P(),
        P("fsdp", None),
        P(),
        P("fsdp", None),
    )
    out_specs = P("fsdp", "sp", None)
    return jax.shard_map(shards, mesh=mesh, in_specs=in_specs, out_specs=out_specs, check_vma=False)
```

```python
import jax
import jax.numpy as jnp
from jax import lax
from jax.experimental import pallas as pl
from jax.experimental.pallas import tpu as pltpu
from jax.sharding import PartitionSpec as P

QH = 32
KVH = 8
HD = 128
D = 5120
T = 256
NDOC = 16
RATIO = QH // KVH
ROWS = D // 16
QUART = ROWS // 4
WIN = 5 * T
EPS = 1e-06
LOG2E = 1.4426950408889634
MESH = pl.DeviceIdType.MESH

YA, ZA, YB, XC, EC, XP, ZU, ZD, ZT = 0, 3, 4, 7, 10, 12, 13, 14, 15
KINDS = 16


RUNS = (
    ("A0", "B0", "A1", "B1", "M0", "A2.0", "C0", "C2.0", "N0", "A2", "A2.1", "C1", "B2", "C2.1", "A3", "E1.0", "E2.0",),
    ("C2", "A2.2", "B3", "E1.1", "E2.1", "A2.3", "C2.2", "V0",),
    ("A4", "E1.2", "B4", "A5", "C3", "E2.2", "A6", "V1", "E1.3", "A7", "C2.3", "B5",),
    ("A2.4", "C4", "A2.5", "E2.3", "V2", "C2.4", "B6",),
    ("C5", "E1.4", "E2.4", "B7", "C2.5", "V3",),
    ("A2.6", "C6", "E1.5", "A2.7", "E2.5", "C2.6", "E1.6", "V4",),
    ("C7", "C2.7", "E2.6", "V5", "E1.7",),
    ("V6", "E2.7",),
    ("V7",),
)


def kernel(
    dl_ref, hid_hbm, q_hbm, gain_ref, w_hbm, vb_ref, out_hbm,
    wbuf, nbuf, qbuf, kvbuf, bias, obuf,
    w_sem, in_sem, out_sem, send, recv,
):
    f = lax.axis_index("fsdp")
    s = lax.axis_index("sp")
    y, zl, c = f // 4, lax.rem(f // 2, 2), lax.rem(f, 2)
    x, zh = s // 4, lax.rem(s, 4)

    def dev(yy, zz, cc, xx, hh):
        return {"fsdp": (yy * 2 + zz) * 2 + cc, "sp": xx * 4 + hh}

    def y_at(d):
        return dev(lax.rem(y + d, 4), zl, c, x, zh)

    def x_at(d):
        return dev(y, zl, c, lax.rem(x + d, 4), zh)

    def h_at(d):
        return dev(y, zl, c, x, lax.rem(zh + d, 4))

    z_pair = dev(y, 1 - zl, c, x, zh)
    z_beside = lax.rem(zh + 3 + 2 * zl, 4)
    z_other = dev(y, 1 - zl, c, x, z_beside)
    core_pair = dev(y, zl, 1 - c, x, zh)
    quarter = pl.ds(pl.multiple_of(x * QUART, 16), QUART)

    def remote(src, dst, kind, h, device):
        return pltpu.make_async_remote_copy(
            src_ref=src,
            dst_ref=dst,
            send_sem=send.at[kind, h],
            recv_sem=recv.at[kind, h],
            device_id=device,
            device_id_type=MESH,
        )

    def ya(h, d):
        own = wbuf.at[h, y, zl, c]
        return remote(own, own, YA + d - 1, h, y_at(d))

    def za(h):
        part = wbuf.at[h, y, zl, c, quarter]
        return remote(part, part, ZA, h, dev(y, 1 - zl, c, x, jnp.where(lax.rem(h, 2) == 0, zh, z_beside)))

    def yb(h, d):
        part = wbuf.at[h, y, 1 - zl, c, quarter]
        return remote(part, part, YB + d - 1, h, y_at(d))

    def xc(h, d):
        part = wbuf.at[h, :, 1 - zl, c, quarter]
        return remote(part, part, XC + d - 1, h, x_at(d))

    def ec(h, other):
        part = wbuf.at[h, :, 1 - zl if other else zl, c]
        return remote(part, part, EC + other, h, core_pair)

    def xp(h):
        return remote(kvbuf.at[h, 4], kvbuf.at[h, 0], XP, h, x_at(1))

    def zu(h):
        return remote(kvbuf.at[h, jnp.where(zh < 3, 4, 0)], kvbuf.at[h, 3], ZU, h, h_at(1))

    def zd(h):
        return remote(kvbuf.at[h, jnp.where(zh > 0, 0, 4)], kvbuf.at[h, 1], ZD, h, h_at(3))

    def zt(h):
        return remote(kvbuf.at[h, jnp.where(zh < 2, 4, 0)], kvbuf.at[h, 2], ZT, h, h_at(2))

    def w_local(h, part):
        columns = pl.ds(pl.multiple_of(part * KVH * HD + h * HD, HD), HD)
        return pltpu.make_async_copy(
            w_hbm.at[:, columns],
            wbuf.at[h, y, zl, c, :, pl.ds(part * HD, HD)],
            w_sem.at[part, h],
        )

    def out_copy(h):
        columns = pl.ds(pl.multiple_of(h * RATIO * HD, HD), RATIO * HD)
        return pltpu.make_async_copy(obuf.at[:, columns], out_hbm.at[:, columns], out_sem.at[h])

    hid_copy = pltpu.make_async_copy(hid_hbm, nbuf, in_sem.at[0])
    q_copy = pltpu.make_async_copy(q_hbm, qbuf, in_sem.at[1])

    @pl.loop(0, KVH)
    def _(h):
        w_local(h, 0).start()
        w_local(h, 1).start()

    hid_copy.start()
    q_copy.start()

    barrier = pltpu.get_barrier_semaphore()
    partners = [y_at(1), y_at(2), y_at(3), x_at(1), x_at(2), x_at(3), h_at(1), h_at(2), h_at(3), z_pair, z_other, core_pair]
    for device in partners:
        pl.semaphore_signal(barrier, inc=1, device_id=device, device_id_type=MESH)
    pl.semaphore_wait(barrier, len(partners))

    def start_a(h):
        w_local(h, 0).wait()
        w_local(h, 1).wait()
        za(h).start()
        ya(h, 1).start()
        ya(h, 3).start()

    def start_a2(h):
        ya(h, 2).start()

    def start_b(h):
        za(h).wait_recv()
        for d in (1, 3, 2):
            yb(h, d).start()

    def start_c(h):
        for d in (1, 2, 3):
            yb(h, d).wait_recv()
        xc(h, 1).start()
        xc(h, 3).start()

    def start_c2(h):
        xc(h, 2).start()

    def start_e1(h):
        for d in (1, 2, 3):
            ya(h, d).wait_recv()
        ec(h, 0).start()

    def start_e2(h):
        for d in (1, 2, 3):
            xc(h, d).wait_recv()
        ec(h, 1).start()

    def project(h):
        ec(h, 0).wait_recv()
        ec(h, 1).wait_recv()
        weight = wbuf[h].reshape(D, 2 * HD)
        result = jnp.dot(nbuf[...], weight, preferred_element_type=jnp.float32)
        kvbuf[h, 4, :, pl.ds(0, HD)] = result[:, :HD].astype(jnp.bfloat16)
        kvbuf[h, 4, :, pl.ds(HD, HD)] = (result[:, HD:] + vb_ref[pl.ds(h, 1), :]).astype(jnp.bfloat16)

    def send_own(h):
        xp(h).start()

        @pl.when(zh < 3)
        def _():
            zu(h).start()

        @pl.when(zh < 2)
        def _():
            zt(h).start()

        @pl.when(zh == 0)
        def _():
            zd(h).start()

    def send_previous(h):
        xp(h).wait_recv()

        @pl.when(zh > 0)
        def _():
            zd(h).start()

        @pl.when(zh >= 2)
        def _():
            zt(h).start()

        @pl.when(zh == 3)
        def _():
            zu(h).start()

    def attend(h):
        zu(h).wait_recv()
        zd(h).wait_recv()
        zt(h).wait_recv()
        key = kvbuf[h, :, :, pl.ds(0, HD)].reshape(WIN, HD)
        value = kvbuf[h, :, :, pl.ds(HD, HD)].reshape(WIN, HD)
        for r in range(RATIO):
            columns = pl.ds(pl.multiple_of((h * RATIO + r) * HD, HD), HD)
            scores = lax.dot_general(
                qbuf[:, columns], key, (((1,), (1,)), ((), ())), preferred_element_type=jnp.float32
            )
            scores = scores * (HD**-0.5 * LOG2E) + bias[...]
            highest = jnp.max(scores, axis=-1, keepdims=True)
            probs = jnp.exp2(scores - highest)
            total = jnp.sum(probs, axis=-1, keepdims=True)
            output = jnp.dot(probs.astype(jnp.bfloat16), value, preferred_element_type=jnp.float32)
            obuf[:, columns] = (output / total).astype(jnp.bfloat16)
        out_copy(h).start()

    def normalise(h):
        hid_copy.wait()

        @pl.loop(0, T // 16)
        def _(i):
            rows = pl.ds(pl.multiple_of(i * 16, 16), 16)
            wide = nbuf[rows, :].astype(jnp.float32)
            square = jnp.mean(wide * wide, axis=-1, keepdims=True)
            nbuf[rows, :] = (wide * lax.rsqrt(square + EPS) * gain_ref[...]).astype(jnp.bfloat16)

    def mask(h):
        first = s * T
        query_pos = first + lax.broadcasted_iota(jnp.int32, (T, 1), 0)
        begin = jnp.zeros((T, 1), jnp.int32)
        end = dl_ref[0, 0]
        for d in range(NDOC):
            begin = jnp.where(query_pos >= end, end, begin)
            if d + 1 < NDOC:
                end = end + dl_ref[0, d + 1]
        key_pos = first - 4 * T + lax.broadcasted_iota(jnp.int32, (T, WIN), 1)
        bias[...] = jnp.where((key_pos <= query_pos) & (key_pos >= begin), 0.0, -jnp.inf)

    steps = {
        "A": start_a, "A2.": start_a2, "B": start_b, "C": start_c, "C2.": start_c2,
        "E1.": start_e1, "E2.": start_e2, "V": send_previous, "N": normalise, "M": mask,
    }

    @pl.loop(0, KVH)
    def _(i):
        for k in range(KVH):

            @pl.when(i == k)
            def _(k=k):
                for word in RUNS[k]:
                    steps[word[:-1]](int(word[-1]))

        project(i)
        send_own(i)

    for word in RUNS[KVH]:
        steps[word[:-1]](int(word[-1]))

    q_copy.wait()

    @pl.loop(0, KVH)
    def _(h):
        attend(h)

    @pl.loop(0, KVH)
    def _(h):
        for d in (1, 2, 3):
            ya(h, d).wait_send()
            yb(h, d).wait_send()
            xc(h, d).wait_send()
        za(h).wait_send()
        ec(h, 0).wait_send()
        ec(h, 1).wait_send()
        xp(h).wait_send()
        zu(h).wait_send()
        zd(h).wait_send()

        zt(h).wait_send()
        out_copy(h).wait()


def shards(hidden, queries, norm_gain, kv_weight, value_bias, doc_lengths):
    anywhere = pl.BlockSpec(memory_space=pl.ANY)
    vmem = pl.BlockSpec(memory_space=pltpu.VMEM)
    out = pl.pallas_call(
        kernel,
        out_shape=jax.ShapeDtypeStruct((T, QH * HD), jnp.bfloat16),
        in_specs=[pl.BlockSpec(memory_space=pltpu.SMEM), anywhere, anywhere, vmem, anywhere, vmem],
        out_specs=anywhere,
        scratch_shapes=[
            pltpu.VMEM((KVH, 4, 2, 2, ROWS, 2 * HD), jnp.bfloat16),
            pltpu.VMEM((T, D), jnp.bfloat16),
            pltpu.VMEM((T, QH * HD), jnp.bfloat16),
            pltpu.VMEM((KVH, 5, T, 2 * HD), jnp.bfloat16),
            pltpu.VMEM((T, WIN), jnp.float32),
            pltpu.VMEM((T, QH * HD), jnp.bfloat16),
            pltpu.SemaphoreType.DMA((2, KVH)),
            pltpu.SemaphoreType.DMA((2,)),
            pltpu.SemaphoreType.DMA((KVH,)),
            pltpu.SemaphoreType.DMA((KINDS, KVH)),
            pltpu.SemaphoreType.DMA((KINDS, KVH)),
        ],
        compiler_params=pltpu.CompilerParams(
            collective_id=0, has_side_effects=True, vmem_limit_bytes=60 * 1024 * 1024
        ),
    )(
        doc_lengths,
        hidden[0],
        queries[0],
        norm_gain.reshape(1, D),
        kv_weight,
        value_bias.reshape(KVH, HD),
    )
    return out.reshape(1, T, QH * HD)


def solution(mesh):
    in_specs = (
        P("fsdp", "sp", None),
        P("fsdp", "sp", None),
        P(),
        P("fsdp", None),
        P(),
        P("fsdp", None),
    )
    out_specs = P("fsdp", "sp", None)
    return jax.shard_map(shards, mesh=mesh, in_specs=in_specs, out_specs=out_specs, check_vma=False)
```

```python
import jax
import jax.numpy as jnp
from jax import lax
from jax.experimental import pallas as pl
from jax.experimental.pallas import tpu as pltpu
from jax.sharding import PartitionSpec as P

QH = 32
KVH = 8
HD = 128
D = 5120
T = 256
NDOC = 16
RATIO = QH // KVH
ROWS = D // 16
QUART = ROWS // 4
WIN = 5 * T
EPS = 1e-06
LOG2E = 1.4426950408889634
MESH = pl.DeviceIdType.MESH

YA, ZA, YB, XC, EC, XP, ZU, ZD, ZT = 0, 3, 4, 7, 10, 12, 13, 14, 15
KINDS = 16


RUNS = (
    ("A0", "B0", "A1", "B1", "M0", "A2.0", "C0", "C2.0", "A2", "N0", "A2.1", "C1", "B2", "C2.1", "A3", "A2.2", "E1.0", "E2.0",),
    ("C2", "B3", "C2.2", "E1.1", "E2.1", "A2.3", "A4", "V0",),
    ("E1.2", "B4", "A5", "C3", "E2.2", "A6", "V1", "E1.3", "A7", "C2.3", "B5",),
    ("A2.4", "C4", "A2.5", "E2.3", "V2", "C2.4", "B6",),
    ("C5", "E1.4", "E2.4", "B7", "C2.5", "V3",),
    ("A2.6", "C6", "E1.5", "A2.7", "E2.5", "C2.6", "E1.6", "V4",),
    ("C7", "C2.7", "E2.6", "V5", "E1.7",),
    ("V6", "E2.7",),
    ("V7",),
)


def kernel(
    dl_ref, hid_hbm, q_hbm, gain_ref, w_hbm, vb_ref, out_hbm,
    wbuf, nbuf, qbuf, kvbuf, bias, obuf,
    w_sem, in_sem, out_sem, send, recv,
):
    f = lax.axis_index("fsdp")
    s = lax.axis_index("sp")
    y, zl, c = f // 4, lax.rem(f // 2, 2), lax.rem(f, 2)
    x, zh = s // 4, lax.rem(s, 4)

    def dev(yy, zz, cc, xx, hh):
        return {"fsdp": (yy * 2 + zz) * 2 + cc, "sp": xx * 4 + hh}

    def y_at(d):
        return dev(lax.rem(y + d, 4), zl, c, x, zh)

    def x_at(d):
        return dev(y, zl, c, lax.rem(x + d, 4), zh)

    def h_at(d):
        return dev(y, zl, c, x, lax.rem(zh + d, 4))

    z_pair = dev(y, 1 - zl, c, x, zh)
    z_beside = lax.rem(zh + 3 + 2 * zl, 4)
    z_other = dev(y, 1 - zl, c, x, z_beside)
    core_pair = dev(y, zl, 1 - c, x, zh)
    quarter = pl.ds(pl.multiple_of(x * QUART, 16), QUART)

    def remote(src, dst, kind, h, device):
        return pltpu.make_async_remote_copy(
            src_ref=src,
            dst_ref=dst,
            send_sem=send.at[kind, h],
            recv_sem=recv.at[kind, h],
            device_id=device,
            device_id_type=MESH,
        )

    def ya(h, d):
        own = wbuf.at[h, y, zl, c]
        return remote(own, own, YA + d - 1, h, y_at(d))

    def za(h):
        part = wbuf.at[h, y, zl, c, quarter]
        return remote(part, part, ZA, h, dev(y, 1 - zl, c, x, jnp.where(lax.rem(h, 2) == 0, zh, z_beside)))

    def yb(h, d):
        part = wbuf.at[h, y, 1 - zl, c, quarter]
        return remote(part, part, YB + d - 1, h, y_at(d))

    def xc(h, d):
        part = wbuf.at[h, :, 1 - zl, c, quarter]
        return remote(part, part, XC + d - 1, h, x_at(d))

    def ec(h, other):
        part = wbuf.at[h, :, 1 - zl if other else zl, c]
        return remote(part, part, EC + other, h, core_pair)

    def xp(h):
        return remote(kvbuf.at[h, 4], kvbuf.at[h, 0], XP, h, x_at(1))

    def zu(h):
        return remote(kvbuf.at[h, jnp.where(zh < 3, 4, 0)], kvbuf.at[h, 3], ZU, h, h_at(1))

    def zd(h):
        return remote(kvbuf.at[h, jnp.where(zh > 0, 0, 4)], kvbuf.at[h, 1], ZD, h, h_at(3))

    def zt(h):
        return remote(kvbuf.at[h, jnp.where(zh < 2, 4, 0)], kvbuf.at[h, 2], ZT, h, h_at(2))

    def w_local(h, part):
        columns = pl.ds(pl.multiple_of(part * KVH * HD + h * HD, HD), HD)
        return pltpu.make_async_copy(
            w_hbm.at[:, columns],
            wbuf.at[h, y, zl, c, :, pl.ds(part * HD, HD)],
            w_sem.at[part, h],
        )

    def out_copy(h):
        columns = pl.ds(pl.multiple_of(h * RATIO * HD, HD), RATIO * HD)
        return pltpu.make_async_copy(obuf.at[:, columns], out_hbm.at[:, columns], out_sem.at[h])

    hid_copy = pltpu.make_async_copy(hid_hbm, nbuf, in_sem.at[0])
    q_copy = pltpu.make_async_copy(q_hbm, qbuf, in_sem.at[1])

    @pl.loop(0, KVH)
    def _(h):
        w_local(h, 0).start()
        w_local(h, 1).start()

    hid_copy.start()
    q_copy.start()

    barrier = pltpu.get_barrier_semaphore()
    partners = [y_at(1), y_at(2), y_at(3), x_at(1), x_at(2), x_at(3), h_at(1), h_at(2), h_at(3), z_pair, z_other, core_pair]
    for device in partners:
        pl.semaphore_signal(barrier, inc=1, device_id=device, device_id_type=MESH)
    pl.semaphore_wait(barrier, len(partners))

    def start_a(h):
        w_local(h, 0).wait()
        w_local(h, 1).wait()
        za(h).start()
        ya(h, 1).start()
        ya(h, 3).start()

    def start_a2(h):
        ya(h, 2).start()

    def start_b(h):
        za(h).wait_recv()
        for d in (1, 3, 2):
            yb(h, d).start()

    def start_c(h):
        for d in (1, 2, 3):
            yb(h, d).wait_recv()
        xc(h, 1).start()
        xc(h, 3).start()

    def start_c2(h):
        xc(h, 2).start()

    def start_e1(h):
        for d in (1, 2, 3):
            ya(h, d).wait_recv()
        ec(h, 0).start()

    def start_e2(h):
        for d in (1, 2, 3):
            xc(h, d).wait_recv()
        ec(h, 1).start()

    def project(h):
        ec(h, 0).wait_recv()
        ec(h, 1).wait_recv()
        weight = wbuf[h].reshape(D, 2 * HD)
        result = jnp.dot(nbuf[...], weight, preferred_element_type=jnp.float32)
        kvbuf[h, 4, :, pl.ds(0, HD)] = result[:, :HD].astype(jnp.bfloat16)
        kvbuf[h, 4, :, pl.ds(HD, HD)] = (result[:, HD:] + vb_ref[pl.ds(h, 1), :]).astype(jnp.bfloat16)

    def send_own(h):
        xp(h).start()

        @pl.when(zh < 3)
        def _():
            zu(h).start()

        @pl.when(zh < 2)
        def _():
            zt(h).start()

        @pl.when(zh == 0)
        def _():
            zd(h).start()

    def send_previous(h):
        xp(h).wait_recv()

        @pl.when(zh > 0)
        def _():
            zd(h).start()

        @pl.when(zh >= 2)
        def _():
            zt(h).start()

        @pl.when(zh == 3)
        def _():
            zu(h).start()

    def attend(h):
        zu(h).wait_recv()
        zd(h).wait_recv()
        zt(h).wait_recv()
        key = kvbuf[h, :, :, pl.ds(0, HD)].reshape(WIN, HD)
        value = kvbuf[h, :, :, pl.ds(HD, HD)].reshape(WIN, HD)
        for r in range(RATIO):
            columns = pl.ds(pl.multiple_of((h * RATIO + r) * HD, HD), HD)
            scores = lax.dot_general(
                qbuf[:, columns], key, (((1,), (1,)), ((), ())), preferred_element_type=jnp.float32
            )
            scores = scores * (HD**-0.5 * LOG2E) + bias[...]
            highest = jnp.max(scores, axis=-1, keepdims=True)
            probs = jnp.exp2(scores - highest)
            total = jnp.sum(probs, axis=-1, keepdims=True)
            output = jnp.dot(probs.astype(jnp.bfloat16), value, preferred_element_type=jnp.float32)
            obuf[:, columns] = (output / total).astype(jnp.bfloat16)
        out_copy(h).start()

    def normalise(h):
        hid_copy.wait()

        @pl.loop(0, T // 16)
        def _(i):
            rows = pl.ds(pl.multiple_of(i * 16, 16), 16)
            wide = nbuf[rows, :].astype(jnp.float32)
            square = jnp.mean(wide * wide, axis=-1, keepdims=True)
            nbuf[rows, :] = (wide * lax.rsqrt(square + EPS) * gain_ref[...]).astype(jnp.bfloat16)

    def mask(h):
        first = s * T
        query_pos = first + lax.broadcasted_iota(jnp.int32, (T, 1), 0)
        begin = jnp.zeros((T, 1), jnp.int32)
        end = dl_ref[0, 0]
        for d in range(NDOC):
            begin = jnp.where(query_pos >= end, end, begin)
            if d + 1 < NDOC:
                end = end + dl_ref[0, d + 1]
        key_pos = first - 4 * T + lax.broadcasted_iota(jnp.int32, (T, WIN), 1)
        bias[...] = jnp.where((key_pos <= query_pos) & (key_pos >= begin), 0.0, -jnp.inf)

    steps = {
        "A": start_a, "A2.": start_a2, "B": start_b, "C": start_c, "C2.": start_c2,
        "E1.": start_e1, "E2.": start_e2, "V": send_previous, "N": normalise, "M": mask,
    }

    @pl.loop(0, KVH)
    def _(i):
        for k in range(KVH):

            @pl.when(i == k)
            def _(k=k):
                for word in RUNS[k]:
                    steps[word[:-1]](int(word[-1]))

        project(i)
        send_own(i)

    for word in RUNS[KVH]:
        steps[word[:-1]](int(word[-1]))

    q_copy.wait()

    @pl.loop(0, KVH)
    def _(h):
        attend(h)

    @pl.loop(0, KVH)
    def _(h):
        for d in (1, 2, 3):
            ya(h, d).wait_send()
            yb(h, d).wait_send()
            xc(h, d).wait_send()
        za(h).wait_send()
        ec(h, 0).wait_send()
        ec(h, 1).wait_send()
        xp(h).wait_send()
        zu(h).wait_send()
        zd(h).wait_send()

        zt(h).wait_send()
        out_copy(h).wait()


def shards(hidden, queries, norm_gain, kv_weight, value_bias, doc_lengths):
    anywhere = pl.BlockSpec(memory_space=pl.ANY)
    vmem = pl.BlockSpec(memory_space=pltpu.VMEM)
    out = pl.pallas_call(
        kernel,
        out_shape=jax.ShapeDtypeStruct((T, QH * HD), jnp.bfloat16),
        in_specs=[pl.BlockSpec(memory_space=pltpu.SMEM), anywhere, anywhere, vmem, anywhere, vmem],
        out_specs=anywhere,
        scratch_shapes=[
            pltpu.VMEM((KVH, 4, 2, 2, ROWS, 2 * HD), jnp.bfloat16),
            pltpu.VMEM((T, D), jnp.bfloat16),
            pltpu.VMEM((T, QH * HD), jnp.bfloat16),
            pltpu.VMEM((KVH, 5, T, 2 * HD), jnp.bfloat16),
            pltpu.VMEM((T, WIN), jnp.float32),
            pltpu.VMEM((T, QH * HD), jnp.bfloat16),
            pltpu.SemaphoreType.DMA((2, KVH)),
            pltpu.SemaphoreType.DMA((2,)),
            pltpu.SemaphoreType.DMA((KVH,)),
            pltpu.SemaphoreType.DMA((KINDS, KVH)),
            pltpu.SemaphoreType.DMA((KINDS, KVH)),
        ],
        compiler_params=pltpu.CompilerParams(
            collective_id=0, has_side_effects=True, vmem_limit_bytes=60 * 1024 * 1024
        ),
    )(
        doc_lengths,
        hidden[0],
        queries[0],
        norm_gain.reshape(1, D),
        kv_weight,
        value_bias.reshape(KVH, HD),
    )
    return out.reshape(1, T, QH * HD)


def solution(mesh):
    in_specs = (
        P("fsdp", "sp", None),
        P("fsdp", "sp", None),
        P(),
        P("fsdp", None),
        P(),
        P("fsdp", None),
    )
    out_specs = P("fsdp", "sp", None)
    return jax.shard_map(shards, mesh=mesh, in_specs=in_specs, out_specs=out_specs, check_vma=False)
```
